8 devices in a mesh: dp: 1 (over z), my: 2 (over y), mx: 4 (over x, core).
Axes of the slice: x: 2, y: 2, z: 1, core: 2. Of those that a mesh axis runs over, the one named last changes fastest.
Arguments:
- tokens: bfloat16 [16, 256, 6144], P('dp', None, 'my')
- ln_scale: bfloat16 [6144], P('my')
- w_in: bfloat16 [6144, 43008], P('my', 'mx')
- mlp_bias: bfloat16 [24576], P('mx')
- q_scale: bfloat16 [128], replicated
- k_scale: bfloat16 [128], replicated
- w_out: bfloat16 [30720, 6144], P('mx', 'my')
- attn_out_bias: bfloat16 [6144], P('my')
- mlp_out_bias: bfloat16 [6144], P('my')
Outputs:
- output: bfloat16 [16, 256, 6144], P('dp', None, 'my')
All inputs are finite; a program needn't handle non-finite values.
Results may differ from the reference program's by a relative error of at most 0.01183.
Values are sent between devices in bfloat16 or wider.
A program may use at most 1 GiB of HBM per device.

```python
import jax
import jax.numpy as jnp
from jax import lax

BATCH = 16
SEQ = 256
D = 6144
HEADS = 48
HEAD = 128
FF = 24576
BLOCKS = 4

HEADS_BLK = HEADS // BLOCKS
FF_BLK = FF // BLOCKS
QKV_BLK = HEADS_BLK * HEAD
IN_BLK = 3 * QKV_BLK + FF_BLK


def block_columns(pieces):
    per_block = [one_piece.reshape(D, BLOCKS, one_piece.shape[1] // BLOCKS) for one_piece in pieces]
    return jnp.concatenate(per_block, axis=2).reshape(D, -1)


def block_rows(pieces):
    per_block = [one_piece.reshape(BLOCKS, one_piece.shape[0] // BLOCKS, D) for one_piece in pieces]
    return jnp.concatenate(per_block, axis=1).reshape(-1, D)


def setup_inputs(seed: int = 0, part: int = 0) -> dict:
    root_key = jax.random.key(seed)
    shared_keys = jax.random.split(root_key, 12)
    part_keys = jax.random.split(jax.random.fold_in(root_key, part), 4)
    width_grid = jnp.linspace(-1.0, 1.0, D)
    mean_amp = jax.random.uniform(part_keys[0], (), jnp.float32, minval=0.6, maxval=1.2)
    scale_amp = jax.random.uniform(part_keys[1], (), jnp.float32, minval=0.3, maxval=0.6)
    row_offset = 0.3 * jax.random.normal(part_keys[2], (BATCH, SEQ, 1), jnp.float32)
    base_noise = jax.random.normal(part_keys[3], (BATCH, SEQ, D), jnp.float32)
    tokens = base_noise * jnp.exp(scale_amp * width_grid) + mean_amp * width_grid + row_offset
    in_gain = D ** -0.5
    w_query = jax.random.normal(shared_keys[0], (D, HEADS * HEAD), jnp.float32) * in_gain
    w_key = jax.random.normal(shared_keys[1], (D, HEADS * HEAD), jnp.float32) * in_gain
    w_value = jax.random.normal(shared_keys[2], (D, HEADS * HEAD), jnp.float32) * in_gain
    w_up = jax.random.normal(shared_keys[3], (D, FF), jnp.float32) * in_gain
    w_attn_out = jax.random.normal(shared_keys[4], (HEADS * HEAD, D), jnp.float32) * (HEADS * HEAD) ** -0.5
    w_down = jax.random.normal(shared_keys[5], (FF, D), jnp.float32) * FF ** -0.5
    return {
        'tokens': tokens.astype(jnp.bfloat16),
        'ln_scale': jax.random.uniform(shared_keys[6], (D,), jnp.float32, minval=0.5, maxval=1.5).astype(jnp.bfloat16),
        'w_in': block_columns([w_query, w_key, w_value, w_up]).astype(jnp.bfloat16),
        'mlp_bias': (0.5 * jax.random.normal(shared_keys[7], (FF,), jnp.float32)).astype(jnp.bfloat16),
        'q_scale': jax.random.uniform(shared_keys[8], (HEAD,), jnp.float32, minval=1.2, maxval=2.0).astype(jnp.bfloat16),
        'k_scale': jax.random.uniform(shared_keys[9], (HEAD,), jnp.float32, minval=1.2, maxval=2.0).astype(jnp.bfloat16),
        'w_out': block_rows([w_attn_out, w_down]).astype(jnp.bfloat16),
        'attn_out_bias': (0.3 * jax.random.normal(shared_keys[10], (D,), jnp.float32)).astype(jnp.bfloat16),
        'mlp_out_bias': (0.3 * jax.random.normal(shared_keys[11], (D,), jnp.float32)).astype(jnp.bfloat16),
    }


def norm_last(features, gain_vec):
    centered = features - jnp.mean(features, axis=-1, keepdims=True)
    variance = jnp.mean(jnp.square(centered), axis=-1, keepdims=True)
    return centered * lax.rsqrt(variance + 1e-6) * gain_vec.astype(jnp.float32)


def reference(tokens, ln_scale, w_in, mlp_bias, q_scale, k_scale, w_out, attn_out_bias, mlp_out_bias):
    out_bias = attn_out_bias.astype(jnp.float32) + mlp_out_bias.astype(jnp.float32)
    unit_bias = mlp_bias.reshape(BLOCKS, FF_BLK).astype(jnp.float32)

    def one_image(image_row):
        tok_f32 = image_row.astype(jnp.float32)
        normed = norm_last(tok_f32, ln_scale).astype(jnp.bfloat16)
        projected = jnp.dot(normed, w_in, preferred_element_type=jnp.float32).astype(jnp.bfloat16)
        projected = projected.reshape(SEQ, BLOCKS, IN_BLK)
        head_shape = (SEQ, HEADS, HEAD)
        queries = norm_last(projected[:, :, :QKV_BLK].reshape(head_shape).astype(jnp.float32), q_scale).astype(jnp.bfloat16)
        keys_n = norm_last(projected[:, :, QKV_BLK:2 * QKV_BLK].reshape(head_shape).astype(jnp.float32), k_scale).astype(jnp.bfloat16)
        values = projected[:, :, 2 * QKV_BLK:3 * QKV_BLK].reshape(head_shape)
        logits = jnp.einsum('qhd,khd->hqk', queries.astype(jnp.float32), keys_n.astype(jnp.float32)) * HEAD ** -0.5
        attn_prob = jax.nn.softmax(logits, axis=-1).astype(jnp.bfloat16)
        mixed = jnp.einsum('hqk,khd->qhd', attn_prob.astype(jnp.float32), values.astype(jnp.float32)).astype(jnp.bfloat16)
        mlp_act = jax.nn.gelu(projected[:, :, 3 * QKV_BLK:].astype(jnp.float32) + unit_bias, approximate=False).astype(jnp.bfloat16)
        joined = jnp.concatenate([mixed.reshape(SEQ, BLOCKS, QKV_BLK), mlp_act], axis=2).reshape(SEQ, -1)
        out_f32 = jnp.dot(joined, w_out, preferred_element_type=jnp.float32)
        return (out_f32 + out_bias + tok_f32).astype(jnp.bfloat16)

    return lax.map(one_image, tokens)
```

```python
import functools

import jax
import jax.numpy as jnp
from jax import lax
from jax.experimental import pallas as pl
from jax.sharding import PartitionSpec as P


SHARED_CHUNKS = (1280, 1280)
SPLIT_CHUNKS = (1024, 768)
TOKEN_SPLIT = (6, 8, 8, 8, 7, 6, 6, 5, 4, 3, 3)


def attention_kernel(q_ref, k_ref, v_ref, q_gain_ref, k_gain_ref, out_ref, *, heads, head_dim):
    def normed(ref, gain_ref, cols):
        feat = ref[:, cols].astype(jnp.float32)
        centered = feat - jnp.mean(feat, axis=-1, keepdims=True)
        variance = jnp.mean(jnp.square(centered), axis=-1, keepdims=True)
        return (centered * lax.rsqrt(variance + 1e-6) * gain_ref[...].astype(jnp.float32)).astype(jnp.bfloat16)

    for head in range(heads):
        cols = slice(head * head_dim, (head + 1) * head_dim)
        queries, keys = normed(q_ref, q_gain_ref, cols), normed(k_ref, k_gain_ref, cols)
        logits = lax.dot_general(queries, keys, (((1,), (1,)), ((), ())), preferred_element_type=jnp.float32)
        logits = logits * head_dim ** -0.5
        weights = jnp.exp(logits - jnp.max(logits, axis=-1, keepdims=True))
        probs = (weights / jnp.sum(weights, axis=-1, keepdims=True)).astype(jnp.bfloat16)
        out_ref[:, cols] = jnp.dot(probs, v_ref[:, cols], preferred_element_type=jnp.float32).astype(jnp.bfloat16)


def attention(queries, keys, values, q_scale, k_scale, batch, seq):
    head_dim = q_scale.shape[0]
    heads = queries.shape[1] // head_dim
    image = pl.BlockSpec((seq, heads * head_dim), lambda i: (i, 0))
    gain = pl.BlockSpec((1, head_dim), lambda i: (0, 0))
    cost = pl.CostEstimate(flops=4 * batch * heads * seq * seq * head_dim, bytes_accessed=8 * queries.size,
                           transcendentals=batch * heads * seq * seq)
    return pl.pallas_call(
        functools.partial(attention_kernel, heads=heads, head_dim=head_dim),
        grid=(batch,), in_specs=[image, image, image, gain, gain], out_specs=image,
        out_shape=jax.ShapeDtypeStruct(queries.shape, jnp.bfloat16), cost_estimate=cost,
    )(queries, keys, values, q_scale.reshape(1, -1), k_scale.reshape(1, -1))


def dot(a, b):
    return jnp.dot(a, b, preferred_element_type=jnp.float32)


def rows_of(array, start, size):
    return lax.dynamic_slice(array, (start, 0), (size, array.shape[1]))


def place(array, part, start):
    return lax.dynamic_update_slice(array, part, (start, 0))


def solution(mesh):
    n_my = mesh.shape['my']
    n_mx = mesh.shape['mx']
    assert n_my == 2 and n_mx == 4
    swap = [(0, 1), (1, 0)]
    core_swap = [(0, 1), (1, 0), (2, 3), (3, 2)]
    chip_swap = [(0, 2), (2, 0), (1, 3), (3, 1)]

    def exchange(value):
        return lax.ppermute(value, 'my', swap)

    def local_layer(tokens, ln_scale, w_in, mlp_bias, q_scale, k_scale, w_out, attn_out_bias, mlp_out_bias):
        batch, seq, width = tokens.shape
        rows = batch * seq
        ff_blk = mlp_bias.shape[0]
        qkv_blk = (w_in.shape[1] - ff_blk) // 3
        qkv_half = qkv_blk // 2
        shared, split = sum(SHARED_CHUNKS), sum(SPLIT_CHUNKS)
        assert shared + n_my * split == ff_blk
        mine = lax.axis_index('my')
        other = 1 - mine
        column = lax.axis_index('mx')
        core = column % 2
        tok = tokens.reshape(rows, width)

        def to_core(value):
            return lax.ppermute(value, 'mx', core_swap)

        def to_chip(value):
            return lax.ppermute(value, 'mx', chip_swap)

        gain_peer = exchange(ln_scale)
        share = rows // n_mx
        piece = exchange(rows_of(tok, column * share, share))
        piece_chip = to_chip(piece)
        pieces = [(piece, column), (piece_chip, column ^ 2),
                  (to_core(piece), column ^ 1), (to_core(piece_chip), column ^ 3)]

        def spans(start, sizes):
            starts = [start + sum(sizes[:i]) for i in range(len(sizes))]
            return list(zip(starts, sizes))

        def columns(side):
            heads = [(part * qkv_blk + side * qkv_half, qkv_half) for part in range(3)]
            both = spans(3 * qkv_blk, SHARED_CHUNKS)
            return heads + spans(3 * qkv_blk + shared + side * split, SPLIT_CHUNKS) + both

        def cut(side):
            return [lax.dynamic_slice(w_in, (0, start), (width, size)) for start, size in columns(side)]

        w_peer = [exchange(block) for block in cut(other)]
        w_mine = cut(mine)

        own_f32 = tok.astype(jnp.float32)
        mean_l = jnp.mean(own_f32, axis=-1)
        dev_l = jnp.sum(jnp.square(own_f32 - mean_l[:, None]), axis=-1)
        stats = exchange(jnp.stack([mean_l, dev_l]))
        total = width * n_my
        mean = (0.5 * (mean_l + stats[0]))[:, None]
        var = (dev_l + stats[1] + jnp.square(mean_l - stats[0]) * (0.5 * width)) / total
        inv = lax.rsqrt(var + 1e-6)[:, None]
        z_own = ((own_f32 - mean) * inv * ln_scale.astype(jnp.float32)).astype(jnp.bfloat16)
        z_peer = jnp.zeros((rows, width), jnp.bfloat16)
        for part, owner in pieces:
            start = owner * share
            centered = part.astype(jnp.float32) - rows_of(mean, start, share)
            scaled = centered * rows_of(inv, start, share) * gain_peer.astype(jnp.float32)
            z_peer = place(z_peer, scaled.astype(jnp.bfloat16), start)

        h = []
        for w0, w1 in zip(w_mine, w_peer):
            own = lax.optimization_barrier(dot(z_own, w0))
            h.append((own + dot(z_peer, w1)).astype(jnp.bfloat16))
        attn = attention(h[0], h[1], h[2], q_scale, k_scale, batch, seq)
        attn_peer = exchange(attn)

        units = spans(shared + mine * split, SPLIT_CHUNKS) + spans(0, SHARED_CHUNKS)
        acts = []
        for part, (start, size) in zip(h[3:], units):
            bias = lax.dynamic_slice(mlp_bias, (start,), (size,)).astype(jnp.float32)
            act = jax.nn.gelu(part.astype(jnp.float32) + bias, approximate=False).astype(jnp.bfloat16)
            acts.append(lax.optimization_barrier(act))
        wo_attn = [rows_of(w_out, side * qkv_half, qkv_half) for side in (mine, other)]
        wo_mlp = [rows_of(w_out, qkv_blk + shared + side * split, split) for side in (mine, other)]
        out_bias = attn_out_bias.astype(jnp.float32) + mlp_out_bias.astype(jnp.float32)
        base = lax.optimization_barrier(dot(attn, wo_attn[0]))
        w_own = [rows_of(wo_mlp[0], start, size) for start, size in spans(0, SPLIT_CHUNKS)]
        w_own += [w_out[start:start + size] for start, size in spans(qkv_blk, SHARED_CHUNKS)]
        for part, weights in zip(acts, w_own):
            base = lax.optimization_barrier(base + dot(part, weights))
        acts = acts[:len(SPLIT_CHUNKS)]

        out = z_peer
        low = 0
        for size in TOKEN_SPLIT:
            count = rows * size // 64
            half = count // 2
            act = jnp.concatenate([part[low:low + count] for part in acts], axis=1)
            act_peer = exchange(act)
            heads_peer = dot(attn_peer[low:low + count], wo_attn[1])
            part = base[low:low + count] + (lax.optimization_barrier(heads_peer) if size < 6 else heads_peer)
            part = (part + dot(act_peer, wo_mlp[1])).astype(jnp.bfloat16)
            part = lax.optimization_barrier(part)
            keep, give = core * half, (1 - core) * half
            got = to_core(rows_of(part, give, half))
            pair = (rows_of(part, keep, half).astype(jnp.float32) + got.astype(jnp.float32)).astype(jnp.bfloat16)
            pair_far = to_chip(pair)
            res = pair.astype(jnp.float32) + pair_far.astype(jnp.float32) + out_bias
            res = (res + rows_of(tok, low + keep, half).astype(jnp.float32)).astype(jnp.bfloat16)
            out = place(out, res, low + keep)
            out = place(out, to_core(res), low + give)
            low += count
        return out.reshape(batch, seq, width)


    specs_in = (P('dp', None, 'my'), P('my'), P('my', 'mx'), P('mx'), P(), P(), P('mx', 'my'), P('my'), P('my'))
    return jax.shard_map(local_layer, mesh=mesh, in_specs=specs_in, out_specs=P('dp', None, 'my'), check_vma=False)
```
